8 devices in a mesh: ep: 8 (over z, y, x, core).
Axes of the slice: x: 2, y: 2, z: 1, core: 2. Of those that a mesh axis runs over, the one named last changes fastest.
Arguments:
- x: bfloat16 [32768, 1024], P('ep')
- gate_w: bfloat16 [1024, 32], replicated
- up_w: bfloat16 [32, 1024, 512], P('ep')
- down_w: bfloat16 [32, 512, 1024], P('ep')
- expert_picks: int32 [32, 2048], P('ep')
- loss_w: bfloat16 [32768, 1024], P('ep')
Outputs:
- output 1: bfloat16 [32768, 1024], P('ep')
- output 2: float32 [], replicated
- output 3: bfloat16 [32768, 1024], P('ep')
- output 4: bfloat16 [32, 1024, 512], P('ep')
- output 5: bfloat16 [32, 512, 1024], P('ep')
- output 6: float32 [1024, 32], replicated
All inputs are finite; a program needn't handle non-finite values.
Results may differ from the reference program's by a relative error of at most 0.0107506.
Values are sent between devices in bfloat16 or wider.
A program may use at most 1 GiB of HBM per device.

```python
import functools
import math
import jax
import jax.numpy as jnp
from jax import lax

HIDDEN = 1024
FFN_DIM = 512
EXPERTS = 32
TOK_DEV = 4096
GROUP_DEVS = 8

TOKENS = TOK_DEV * GROUP_DEVS
CAPACITY = 2 * TOKENS // EXPERTS
LOCAL_EXPERTS = EXPERTS // GROUP_DEVS
SHARD_PICKS = CAPACITY // GROUP_DEVS
POOL_SIZE = max(SHARD_PICKS, LOCAL_EXPERTS * SHARD_PICKS // 2)


@jax.custom_vjp
def grad_to_bf16(in_value):
    return in_value


def grad_to_bf16_fwd(in_value):
    return in_value, None


def grad_to_bf16_bwd(residual, cotangent):
    return (cotangent.astype(jnp.bfloat16).astype(jnp.float32),)


grad_to_bf16.defvjp(grad_to_bf16_fwd, grad_to_bf16_bwd)


def draw_picks(base_key):
    perm_keys = jax.random.split(jax.random.fold_in(base_key, 1), GROUP_DEVS)
    shard_perms = jax.vmap(functools.partial(jax.random.permutation, x=TOK_DEV))(perm_keys)
    offsets = jax.random.randint(jax.random.fold_in(base_key, 2), (GROUP_DEVS, GROUP_DEVS), 0, TOK_DEV)
    pool_pos = (jnp.arange(LOCAL_EXPERTS)[:, None] * SHARD_PICKS + jnp.arange(SHARD_PICKS)[None, :]) % POOL_SIZE
    perm_pos = (offsets[:, None, :, None] + pool_pos[None, :, None, :]) % TOK_DEV
    src_ids = jnp.arange(GROUP_DEVS)[None, None, :, None]
    token_ids = src_ids * TOK_DEV + shard_perms[src_ids, perm_pos]
    return token_ids.reshape(EXPERTS, CAPACITY).astype(jnp.int32)


def setup_inputs(seed: int = 0) -> dict:
    key_list = jax.random.split(jax.random.key(seed), 6)
    x = jax.random.normal(key_list[0], (TOKENS, HIDDEN), jnp.float32)
    gate_w = jax.random.normal(key_list[1], (HIDDEN, EXPERTS), jnp.float32) * HIDDEN ** -0.5
    up_w = jax.random.normal(key_list[2], (EXPERTS, HIDDEN, FFN_DIM), jnp.float32) * HIDDEN ** -0.5
    down_w = jax.random.normal(key_list[3], (EXPERTS, FFN_DIM, HIDDEN), jnp.float32) * (EXPERTS / (2.0 * math.sqrt(FFN_DIM)))
    loss_w = jax.random.normal(key_list[5], (TOKENS, HIDDEN), jnp.float32)
    return {'x': x.astype(jnp.bfloat16), 'gate_w': gate_w.astype(jnp.bfloat16), 'up_w': up_w.astype(jnp.bfloat16), 'down_w': down_w.astype(jnp.bfloat16), 'expert_picks': draw_picks(key_list[4]), 'loss_w': loss_w.astype(jnp.bfloat16)}


def mixed_tokens(x_f32, gate_w32, up_w, down_w, expert_picks):
    logits = grad_to_bf16(jnp.dot(x_f32, gate_w32))
    gate_probs = jax.nn.softmax(logits, axis=-1)
    gate_vals = gate_probs[expert_picks, jnp.arange(EXPERTS)[:, None]]

    def one_expert(operands):
        pick_ids, up_one, down_one, gate_one = operands
        tok_rows = grad_to_bf16(x_f32[pick_ids])
        pre_act = grad_to_bf16(jnp.dot(tok_rows, up_one.astype(jnp.float32)))
        hidden_act = jax.nn.gelu(pre_act).astype(jnp.bfloat16)
        expert_out = jnp.dot(hidden_act.astype(jnp.float32), down_one.astype(jnp.float32)).astype(jnp.bfloat16)
        return gate_one[:, None] * expert_out.astype(jnp.float32)

    contrib = lax.map(jax.checkpoint(one_expert), (expert_picks, up_w, down_w, gate_vals))
    return x_f32.at[expert_picks.reshape(-1)].add(contrib.reshape(-1, HIDDEN))


def reference(x, gate_w, up_w, down_w, expert_picks, loss_w):
    loss_scale = 1.0 / math.sqrt(TOKENS * HIDDEN)
    mixed_f32, pullback = jax.vjp(functools.partial(mixed_tokens, expert_picks=expert_picks), x.astype(jnp.float32), gate_w.astype(jnp.float32), up_w, down_w)
    y = mixed_f32.astype(jnp.bfloat16)
    weight_f32 = loss_w.astype(jnp.float32)
    loss = jnp.sum(y.astype(jnp.float32) * weight_f32) * loss_scale
    grad_x, grad_gate, grad_up, grad_down = pullback(weight_f32 * loss_scale)
    return y, loss, grad_x.astype(jnp.bfloat16), grad_up, grad_down, grad_gate
```

```python
import functools
import math
import jax
import jax.numpy as jnp
from jax import lax
from jax.experimental import pallas as pl
from jax.experimental.pallas import tpu as pltpu
from jax.sharding import PartitionSpec as P


F32, BF16 = jnp.float32, jnp.bfloat16
LANES = 128
CHUNK = 512
MIB = 2**20


def as_tiles(ref, cols):
    return ref.reshape(ref.shape[0] * LANES // (8 * cols), cols // LANES, 8, LANES)


def put_rows(ref, start, value):
    rows, cols = value.shape
    tiles = as_tiles(ref, cols)
    for c in range(cols // LANES):
        tiles[pl.ds(start // 8, rows // 8), c] = value[:, c * LANES:(c + 1) * LANES].reshape(rows // 8, 8, LANES)


def get_rows(ref, start, rows, cols):
    tiles = as_tiles(ref, cols)
    parts = [tiles[pl.ds(start // 8, rows // 8), c].reshape(rows, LANES) for c in range(cols // LANES)]
    return jnp.concatenate(parts, axis=1)


def row_base(row):
    return ((row >> 3) << 6) | (row & 7)


def gather_body(idx, *refs, num_src, rows, block):
    srcs = refs[:num_src]
    out, src32, stage, buf, sem = refs[num_src:]
    step = pl.program_id(0)
    chunks = rows // CHUNK

    @pl.when(step == 0)
    def _():
        def load(k):
            src = srcs[k] if num_src > 1 else srcs[0].at[pl.ds(k * CHUNK, CHUNK)]
            return pltpu.make_async_copy(src, buf.at[k % 2], sem.at[k % 2])

        load(0).start()
        for k in range(chunks):
            if k + 1 < chunks:
                load(k + 1).start()
            load(k).wait()
            put_rows(src32, k * CHUNK, buf[k % 2].astype(F32))

    unroll = 16

    def body(i, carry):
        vals = [src32[pl.ds(idx[step * block + i * unroll + j], 8, stride=8), :] for j in range(unroll)]
        for j in range(unroll):
            stage[pl.ds(i * (unroll * 8) + (j // 8) * 64 + j % 8, 8, stride=8), :] = vals[j]
        return carry

    lax.fori_loop(0, block // unroll, body, 0)
    out[...] = get_rows(stage, 0, block, out.shape[1]).astype(BF16)


def gather_rows(idx, srcs, num_out):
    rows, cols = sum(s.shape[0] for s in srcs), srcs[0].shape[1]
    block = 512
    return pl.pallas_call(
        functools.partial(gather_body, num_src=len(srcs), rows=rows, block=block),
        grid_spec=pltpu.PrefetchScalarGridSpec(
            num_scalar_prefetch=1, grid=(num_out // block,),
            in_specs=[pl.BlockSpec(memory_space=pl.ANY)] * len(srcs),
            out_specs=pl.BlockSpec((block, cols), lambda i, idx: (i, 0)),
            scratch_shapes=[pltpu.VMEM((rows * 8, LANES), F32), pltpu.VMEM((block * 8, LANES), F32),
                            pltpu.VMEM((2, CHUNK, cols), BF16), pltpu.SemaphoreType.DMA((2,))]),
        out_shape=jax.ShapeDtypeStruct((num_out, cols), BF16),
        compiler_params=pltpu.CompilerParams(dimension_semantics=("arbitrary",), vmem_limit_bytes=40 * MIB),
        cost_estimate=pl.CostEstimate(flops=num_out * 1_000_000, bytes_accessed=num_out * cols * 4, transcendentals=0))(idx, *srcs)


def dot(a, b):
    return lax.dot_general(a, b, (((1,), (0,)), ((), ())), preferred_element_type=F32)


def dot_nt(a, b):
    return lax.dot_general(a, b, (((1,), (1,)), ((), ())), preferred_element_type=F32)


def dot_tn(a, b):
    return lax.dot_general(a, b, (((0,), (0,)), ((), ())), preferred_element_type=F32)


def softmax_rows(x_rows, gate_pad, experts):
    logits = dot(x_rows, gate_pad)
    lane = lax.broadcasted_iota(jnp.int32, logits.shape, 1)
    live = lane < experts
    logits = jnp.where(live, logits, -jnp.inf)
    e = jnp.exp(logits - jnp.max(logits, axis=1, keepdims=True))
    return e / jnp.sum(e, axis=1, keepdims=True), lane


def gelu_parts(a):
    c = math.sqrt(2.0 / math.pi)
    sq = a * a
    t = jnp.tanh(c * (a + 0.044715 * (sq * a)))
    half = 0.5 * (1.0 + t)
    return a * half, half + (0.5 * a) * (1.0 - t * t) * (c + (3.0 * 0.044715 * c) * sq)


def owner_body(ids, x_ref, r_ref, w1_ref, w2_ref, gate_ref, *refs, first, experts, scale):
    h_ref, g_ref, aux_ref = refs[-3:]
    expert = ids[first + pl.program_id(0)]
    x_rows = x_ref[...]
    w1, w2 = w1_ref[0], w2_ref[0]
    probs, lane = softmax_rows(x_rows, gate_ref[...], experts)
    gate = jnp.sum(jnp.where(lane == expert, probs, 0.0), axis=1, keepdims=True)
    act, slope = gelu_parts(dot(x_rows, w1))
    h = dot(act.astype(BF16), w2).astype(BF16)
    dy = r_ref[...].astype(F32) * scale
    gate_grad = jnp.sum(dy * h.astype(F32), axis=1, keepdims=True)
    dh = (gate * dy).astype(BF16)
    du = dot_nt(dh, w2).astype(BF16)
    da = (slope * du.astype(F32)).astype(BF16)
    h_ref[...] = h
    g_ref[...] = dot_nt(da, w1).astype(BF16)
    aux_ref[...] = jnp.where(lane == expert, gate_grad, jnp.where(lane == 64, gate, 0.0))


def owner_group(ids, picked_x, picked_r, w1, w2, gate_pad, bufs, first, picks, experts, scale):
    num = w1.shape[0]
    cols, width = w1.shape[1], w1.shape[2]
    total = picked_x.shape[0]
    rows = lambda i, ids: (first + i, 0)
    weight = lambda i, ids: (i, 0, 0)
    in_specs = [pl.BlockSpec((picks, cols), rows), pl.BlockSpec((picks, cols), rows),
                pl.BlockSpec((1, cols, width), weight), pl.BlockSpec((1, width, cols), weight),
                pl.BlockSpec(gate_pad.shape, lambda i, ids: (0, 0))]
    alias = {}
    if bufs:
        in_specs += [pl.BlockSpec(memory_space=pl.ANY)] * 3
        alias = {6: 0, 7: 1, 8: 2}
    return pl.pallas_call(
        functools.partial(owner_body, first=first, experts=experts, scale=scale),
        grid_spec=pltpu.PrefetchScalarGridSpec(
            num_scalar_prefetch=1, grid=(num,), in_specs=in_specs,
            out_specs=[pl.BlockSpec((picks, cols), rows), pl.BlockSpec((picks, cols), rows),
                       pl.BlockSpec((picks, LANES), rows)]),
        out_shape=[jax.ShapeDtypeStruct((total, cols), BF16), jax.ShapeDtypeStruct((total, cols), BF16),
                   jax.ShapeDtypeStruct((total, LANES), F32)],
        input_output_aliases=alias,
        compiler_params=pltpu.CompilerParams(dimension_semantics=("arbitrary",), vmem_limit_bytes=40 * MIB),
        cost_estimate=pl.CostEstimate(flops=num * 1_000_000_000, bytes_accessed=num * 4 * MIB, transcendentals=0))(ids, picked_x, picked_r, w1, w2, gate_pad, *bufs)


def expert_body(ids, x_ref, r_ref, w1_ref, w2_ref, gate_ref, up_ref, down_ref, up_acc, down_acc, *, experts, scale):
    expert = ids[pl.program_id(0)]
    step = pl.program_id(1)
    x_rows = x_ref[...]
    w1, w2 = w1_ref[0], w2_ref[0]
    probs, lane = softmax_rows(x_rows, gate_ref[...], experts)
    gate = jnp.sum(jnp.where(lane == expert, probs, 0.0), axis=1, keepdims=True)
    act, slope = gelu_parts(dot(x_rows, w1))
    dh = (gate * (r_ref[...].astype(F32) * scale)).astype(BF16)
    du = dot_nt(dh, w2).astype(BF16)
    da = (slope * du.astype(F32)).astype(BF16)

    @pl.when(step == 0)
    def _():
        up_acc[...] = jnp.zeros_like(up_acc)
        down_acc[...] = jnp.zeros_like(down_acc)

    down_acc[...] += dot_tn(act.astype(BF16), dh)
    up_acc[...] += dot_tn(x_rows, da)

    @pl.when(step == pl.num_programs(1) - 1)
    def _():
        up_ref[0] = up_acc[...].astype(BF16)
        down_ref[0] = down_acc[...].astype(BF16)


def expert_grads(ids, rows_x, rows_r, w1, w2, gate_pad, experts, scale):
    num, cols, width = w1.shape
    block = 512
    steps = rows_x.shape[0] // num // block
    rows = lambda e, i, ids: (e * steps + i, 0)
    weight = lambda e, i, ids: (e, 0, 0)
    return pl.pallas_call(
        functools.partial(expert_body, experts=experts, scale=scale),
        grid_spec=pltpu.PrefetchScalarGridSpec(
            num_scalar_prefetch=1, grid=(num, steps),
            in_specs=[pl.BlockSpec((block, cols), rows), pl.BlockSpec((block, cols), rows),
                      pl.BlockSpec((1, cols, width), weight), pl.BlockSpec((1, width, cols), weight),
                      pl.BlockSpec(gate_pad.shape, lambda e, i, ids: (0, 0))],
            out_specs=[pl.BlockSpec((1, cols, width), weight), pl.BlockSpec((1, width, cols), weight)],
            scratch_shapes=[pltpu.VMEM((cols, width), F32), pltpu.VMEM((width, cols), F32)]),
        out_shape=[jax.ShapeDtypeStruct(w1.shape, BF16), jax.ShapeDtypeStruct(w2.shape, BF16)],
        compiler_params=pltpu.CompilerParams(dimension_semantics=("arbitrary", "arbitrary"), vmem_limit_bytes=48 * MIB),
        cost_estimate=pl.CostEstimate(flops=45_000_000_000, bytes_accessed=48 * MIB, transcendentals=0),
        name="expert_grads")(ids, rows_x, rows_r, w1, w2, gate_pad)


def combine_body(idx, tok, x_ref, r_ref, h_ref, g_ref, aux_ref, gate_ref, y_ref, gx_ref, part_ref,
                 y_acc, g_acc, s_acc, y_stage, g_stage, *, chunks, blocks, experts, scale):
    step = pl.program_id(0)
    picks = h_ref.shape[0]

    @pl.when(step < chunks)
    def _():
        put_rows(y_acc, step * CHUNK, x_ref[...].astype(F32))
        put_rows(g_acc, step * CHUNK, r_ref[...].astype(F32) * scale)
        s_acc[pl.ds(step * CHUNK, CHUNK), :] = jnp.zeros((CHUNK, LANES), F32)

    @pl.when((step >= chunks) & (step < chunks + blocks))
    def _():
        put_rows(y_stage, 0, h_ref[...].astype(F32) * aux_ref[:, 64:65])
        put_rows(g_stage, 0, g_ref[...].astype(F32))
        base = (step - chunks) * picks
        unroll = 8

        def body(i, carry):
            at = [idx[base + i * unroll + j] for j in range(unroll)]
            row = [tok[base + i * unroll + j] for j in range(unroll)]
            ys = [y_acc[pl.ds(at[j], 8, stride=8), :] + y_stage[pl.ds(i * 64 + j, 8, stride=8), :] for j in range(unroll)]
            gs = [g_acc[pl.ds(at[j], 8, stride=8), :] + g_stage[pl.ds(i * 64 + j, 8, stride=8), :] for j in range(unroll)]
            ss = [s_acc[pl.ds(row[j], 1), :] + aux_ref[pl.ds(i * unroll + j, 1), :] for j in range(unroll)]
            for j in range(unroll):
                y_acc[pl.ds(at[j], 8, stride=8), :] = ys[j]
                g_acc[pl.ds(at[j], 8, stride=8), :] = gs[j]
                s_acc[pl.ds(row[j], 1), :] = ss[j]
            return carry

        lax.fori_loop(0, picks // unroll, body, 0)

    @pl.when(step >= chunks + blocks)
    def _():
        start = (step - chunks - blocks) * CHUNK
        cols = x_ref.shape[1]
        x_rows = x_ref[...]
        probs, lane = softmax_rows(x_rows, gate_ref[...], experts)
        dprobs = jnp.where(lane < experts, s_acc[pl.ds(start, CHUNK), :], 0.0)
        dlogits = (probs * (dprobs - jnp.sum(probs * dprobs, axis=1, keepdims=True))).astype(BF16)
        gx_ref[...] = (get_rows(g_acc, start, CHUNK, cols) + dot_nt(dlogits, gate_ref[...])).astype(BF16)
        y = get_rows(y_acc, start, CHUNK, cols).astype(BF16)
        y_ref[...] = y
        prod = y.astype(F32) * r_ref[...].astype(F32)

        @pl.when(step == chunks + blocks)
        def _():
            part_ref[...] = jnp.zeros_like(part_ref)

        part_ref[0:experts, :] += dot_tn(dlogits, x_rows)[0:experts]
        part_ref[experts:experts + 8, :] += prod.reshape(CHUNK // 8, 8, cols).sum(axis=0)


def combine(idx, tok, x, loss_w, h, g, aux, gate_pad, picks, experts, scale):
    tokens, cols = x.shape
    chunks, blocks = tokens // CHUNK, h.shape[0] // picks
    token_map = lambda i, idx, tok: (jnp.where(i < chunks, i, jnp.maximum(i - chunks - blocks, 0)), 0)
    block_map = lambda i, idx, tok: (jnp.clip(i - chunks, 0, blocks - 1), 0)
    out_map = lambda i, idx, tok: (jnp.maximum(i - chunks - blocks, 0), 0)
    whole = lambda i, idx, tok: (0, 0)
    return pl.pallas_call(
        functools.partial(combine_body, chunks=chunks, blocks=blocks, experts=experts, scale=scale),
        grid_spec=pltpu.PrefetchScalarGridSpec(
            num_scalar_prefetch=2, grid=(2 * chunks + blocks,),
            in_specs=[pl.BlockSpec((CHUNK, cols), token_map), pl.BlockSpec((CHUNK, cols), token_map),
                      pl.BlockSpec((picks, cols), block_map), pl.BlockSpec((picks, cols), block_map),
                      pl.BlockSpec((picks, LANES), block_map), pl.BlockSpec(gate_pad.shape, whole)],
            out_specs=[pl.BlockSpec((CHUNK, cols), out_map), pl.BlockSpec((CHUNK, cols), out_map),
                       pl.BlockSpec((experts + 8, cols), whole)],
            scratch_shapes=[pltpu.VMEM((tokens * 8, LANES), F32), pltpu.VMEM((tokens * 8, LANES), F32),
                            pltpu.VMEM((tokens, LANES), F32),
                            pltpu.VMEM((picks * 8, LANES), F32), pltpu.VMEM((picks * 8, LANES), F32)]),
        out_shape=[jax.ShapeDtypeStruct(x.shape, BF16), jax.ShapeDtypeStruct(x.shape, BF16),
                   jax.ShapeDtypeStruct((experts + 8, cols), F32)],
        compiler_params=pltpu.CompilerParams(dimension_semantics=("arbitrary",), vmem_limit_bytes=58 * MIB),
        cost_estimate=pl.CostEstimate(flops=50_000_000_000, bytes_accessed=64 * MIB, transcendentals=0),
        name="combine")(idx, tok, x, loss_w, h, g, aux, gate_pad)


def rank_picks(tok, tokens, distinct):
    side = 64
    steps = jnp.arange(side)
    hi = (tok // side)[..., None] == steps
    lo = (tok % side)[..., None] == steps
    hist = jnp.einsum('tph,tpl->thl', hi.astype(BF16), lo.astype(BF16), preferred_element_type=F32)
    seen = (hist > 0).astype(BF16)
    upto = (steps[:, None] <= steps[None, :]).astype(BF16)
    within = jnp.einsum('thl,lk->thk', seen, upto, preferred_element_type=F32)
    before = jnp.sum(jnp.where(steps[None, :, None] > steps[None, None, :], within[:, None, :, -1], 0.0), axis=-1)
    count = within + before[..., None]
    row = jnp.einsum('tph,thl->tpl', hi.astype(BF16), within.astype(BF16), preferred_element_type=F32)
    start = jnp.sum(jnp.where(hi, before[:, None, :], 0.0), axis=-1)
    place = (jnp.sum(jnp.where(lo, row, 0.0), axis=-1) + start - 1.0).astype(jnp.int32)
    flat = count.reshape(tok.shape[0], 1, tokens)
    listed = jnp.sum((flat <= jnp.arange(distinct, dtype=F32)[None, :, None]).astype(jnp.int32), axis=-1)
    return listed, place


def after(value, *earlier):
    return lax.optimization_barrier((value, *earlier))[0]


def solution(mesh):
    group = mesh.shape['ep']

    def permute(value, mask):
        return lax.ppermute(value, 'ep', [(i, i ^ mask) for i in range(group)])

    def dispatch(rows):
        size = rows.shape[0] // group
        return [rows[:size]] + [permute(rows[m * size:(m + 1) * size], m) for m in range(1, group)]

    def device_step(x, gate_w, up_w, down_w, expert_picks, loss_w):
        tokens, cols = x.shape
        experts = gate_w.shape[1]
        local, capacity = expert_picks.shape
        picks = capacity // group
        distinct = local * picks // 2
        scale = 1.0 / math.sqrt(tokens * group * cols)
        me = lax.axis_index('ep')
        order = me ^ jnp.arange(group)
        gate_pad = jnp.pad(gate_w, ((0, 0), (0, LANES - experts)))

        wanted = expert_picks.reshape(local, group, picks)
        asked = lax.all_to_all(wanted, 'ep', 1, 1, tiled=True) - me * tokens
        asked = jnp.take(asked, order, axis=1).transpose(1, 0, 2)
        wanted = (jnp.take(wanted, order, axis=1) - (order * tokens)[None, :, None]).transpose(1, 0, 2)

        half = local // 2
        part_a = after((up_w[:half], down_w[:half]), asked)
        xa, ya = [permute(v, 2) for v in part_a], [permute(v, 4) for v in part_a]
        partner = [permute(up_w, 1), permute(down_w, 1)]

        send_list, _ = rank_picks(asked.reshape(group, -1), tokens, distinct)
        send_idx = row_base(send_list).reshape(-1)
        send_x = gather_rows(send_idx, [x], group * distinct)
        send_r = gather_rows(after(send_idx, send_x), [loss_w], group * distinct)
        got_x, got_r = dispatch(send_x), dispatch(send_r)

        part_b = after((up_w[half:], down_w[half:]), send_r)
        xb, yb = [permute(v, 2) for v in part_b], [permute(v, 4) for v in part_b]

        own_tok = asked.reshape(-1)
        own_idx = row_base(own_tok)
        own_ids = (order[:, None] * local + jnp.arange(local)[None, :]).reshape(-1)
        picked_x = gather_rows(after(own_idx, send_r), [x], experts * picks)
        picked_r = gather_rows(after(own_idx, picked_x), [loss_w], experts * picks)

        def relay(vx, vy):
            return [permute(vx[0], 4), permute(vy[1], 2)]

        da, db = relay(xa, ya), relay(xb, yb)
        xa1, ya1, xb1, yb1, da1, db1 = ([permute(v, 1) for v in vs] for vs in (xa, ya, xb, yb, da, db))

        def owner(bufs, first, weights):
            ids = after(own_ids, bufs[2]) if bufs else own_ids
            return owner_group(ids, picked_x, picked_r, *weights, gate_pad, bufs, first, picks, experts, scale)

        bufs = owner([], 0, (up_w, down_w))
        bufs = owner(bufs, local, partner)
        for m, weights in ((2, xa), (4, ya), (3, xa1), (5, ya1)):
            bufs = owner(bufs, m * local, weights)

        _, place = rank_picks(wanted.reshape(group, -1), tokens, distinct)
        rows_idx = row_base(place.reshape(group, local, picks) + jnp.arange(group)[:, None, None] * distinct)
        rows_idx = rows_idx.transpose(1, 0, 2).reshape(-1)
        my_ids = me * local + jnp.arange(local)
        rows_x = gather_rows(after(rows_idx, bufs[2]), got_x, local * capacity)
        rows_r = gather_rows(after(rows_idx, rows_x), got_r, local * capacity)
        grad_up, grad_down = expert_grads(my_ids, rows_x, rows_r, up_w, down_w, gate_pad, experts, scale)

        own_ids = after(own_ids, grad_down)
        for m, weights in ((2, xb), (4, yb), (3, xb1), (5, yb1)):
            bufs = owner(bufs, m * local + half, weights)
        for m, start, weights in ((6, 0, da), (7, 0, da1), (6, half, db), (7, half, db1)):
            bufs = owner(bufs, m * local + start, weights)

        y, grad_x, part = combine(own_idx, own_tok, x, loss_w, *bufs, gate_pad, picks, experts, scale)
        for mask in (1, 2, 4):
            part = part + permute(part, mask)
        return y, jnp.sum(part[experts:]) * scale, grad_x, grad_up, grad_down, part[:experts].T

    return jax.shard_map(device_step, mesh=mesh,
                         in_specs=(P('ep'), P(), P('ep'), P('ep'), P('ep'), P('ep')),
                         out_specs=(P('ep'), P(), P('ep'), P('ep'), P('ep'), P()),
                         check_vma=False)
```

```python
import functools
import math
import jax
import jax.numpy as jnp
from jax import lax
from jax.experimental import pallas as pl
from jax.experimental.pallas import tpu as pltpu
from jax.sharding import PartitionSpec as P


F32, BF16 = jnp.float32, jnp.bfloat16
LANES = 128
CHUNK = 512
MIB = 2**20


def as_tiles(ref, cols):
    return ref.reshape(ref.shape[0] * LANES // (8 * cols), cols // LANES, 8, LANES)


def put_rows(ref, start, value):
    rows, cols = value.shape
    tiles = as_tiles(ref, cols)
    for c in range(cols // LANES):
        tiles[pl.ds(start // 8, rows // 8), c] = value[:, c * LANES:(c + 1) * LANES].reshape(rows // 8, 8, LANES)


def get_rows(ref, start, rows, cols, first=0, wide=None):
    tiles = as_tiles(ref, cols)
    spans = range(first // LANES, (first + (wide or cols)) // LANES)
    return jnp.concatenate([tiles[pl.ds(start // 8, rows // 8), c].reshape(rows, LANES) for c in spans], axis=1)


def row_base(row):
    return ((row >> 3) << 6) | (row & 7)


def gather_body(idx, *refs, num_src, rows, block):
    srcs = refs[:num_src]
    out, src32, stage, buf, sem = refs[num_src:]
    step = pl.program_id(0)
    chunks = rows // CHUNK

    @pl.when(step == 0)
    def _():
        def load(k):
            src = srcs[k] if num_src > 1 else srcs[0].at[pl.ds(k * CHUNK, CHUNK)]
            return pltpu.make_async_copy(src, buf.at[k % 2], sem.at[k % 2])

        load(0).start()
        for k in range(chunks):
            if k + 1 < chunks:
                load(k + 1).start()
            load(k).wait()
            put_rows(src32, k * CHUNK, buf[k % 2].astype(F32))

    unroll = 16

    def body(i, carry):
        vals = [src32[pl.ds(idx[step * block + i * unroll + j], 8, stride=8), :] for j in range(unroll)]
        for j in range(unroll):
            stage[pl.ds(i * (unroll * 8) + (j // 8) * 64 + j % 8, 8, stride=8), :] = vals[j]
        return carry

    lax.fori_loop(0, block // unroll, body, 0)
    out[...] = get_rows(stage, 0, block, out.shape[1]).astype(BF16)


def gather_rows(idx, srcs, num_out):
    rows, cols = sum(s.shape[0] for s in srcs), srcs[0].shape[1]
    block = 512
    return pl.pallas_call(
        functools.partial(gather_body, num_src=len(srcs), rows=rows, block=block),
        grid_spec=pltpu.PrefetchScalarGridSpec(
            num_scalar_prefetch=1, grid=(num_out // block,),
            in_specs=[pl.BlockSpec(memory_space=pl.ANY)] * len(srcs),
            out_specs=pl.BlockSpec((block, cols), lambda i, idx: (i, 0)),
            scratch_shapes=[pltpu.VMEM((rows * 8, LANES), F32), pltpu.VMEM((block * 8, LANES), F32),
                            pltpu.VMEM((2, CHUNK, cols), BF16), pltpu.SemaphoreType.DMA((2,))]),
        out_shape=jax.ShapeDtypeStruct((num_out, cols), BF16),
        compiler_params=pltpu.CompilerParams(dimension_semantics=("arbitrary",), vmem_limit_bytes=40 * MIB),
        cost_estimate=pl.CostEstimate(flops=num_out * 1_000_000, bytes_accessed=num_out * cols * 4, transcendentals=0))(idx, *srcs)


def dot(a, b):
    return lax.dot_general(a, b, (((1,), (0,)), ((), ())), preferred_element_type=F32)


def dot_nt(a, b):
    return lax.dot_general(a, b, (((1,), (1,)), ((), ())), preferred_element_type=F32)


def dot_tn(a, b):
    return lax.dot_general(a, b, (((0,), (0,)), ((), ())), preferred_element_type=F32)


def softmax_rows(x_rows, gate_pad, experts):
    logits = dot(x_rows, gate_pad)
    lane = lax.broadcasted_iota(jnp.int32, logits.shape, 1)
    live = lane < experts
    logits = jnp.where(live, logits, -jnp.inf)
    e = jnp.exp(logits - jnp.max(logits, axis=1, keepdims=True))
    return e / jnp.sum(e, axis=1, keepdims=True), lane


def gelu_parts(a):
    c = math.sqrt(2.0 / math.pi)
    sq = a * a
    t = jnp.tanh(c * (a + 0.044715 * (sq * a)))
    half = 0.5 * (1.0 + t)
    return a * half, half + (0.5 * a) * (1.0 - t * t) * (c + (3.0 * 0.044715 * c) * sq)


def owner_expert(x_rows, r_rows, w1, w2, gate_pad, expert, experts, scale):
    probs, lane = softmax_rows(x_rows, gate_pad, experts)
    gate = jnp.sum(jnp.where(lane == expert, probs, 0.0), axis=1, keepdims=True)
    act, slope = gelu_parts(dot(x_rows, w1))
    h = dot(act.astype(BF16), w2).astype(BF16)
    dy = r_rows.astype(F32) * scale
    gate_grad = jnp.sum(dy * h.astype(F32), axis=1, keepdims=True)
    dh = (gate * dy).astype(BF16)
    du = dot_nt(dh, w2).astype(BF16)
    da = (slope * du.astype(F32)).astype(BF16)
    aux = jnp.where(lane == expert, gate_grad, jnp.where(lane == 64, gate, 0.0))
    return h, dot_nt(da, w1).astype(BF16), aux


def owner_body(ids, x_ref, r_ref, gate_ref, *refs, first, per, num_pairs, experts, scale):
    weights = refs[:2 * num_pairs]
    h_ref, g_ref, aux_ref = refs[-3:]
    step = pl.program_id(0)

    def one_expert(w1_ref, w2_ref):
        h_ref[...], g_ref[...], aux_ref[...] = owner_expert(
            x_ref[...], r_ref[...], w1_ref[0], w2_ref[0], gate_ref[...], ids[first + step], experts, scale)

    for k in range(num_pairs):
        if num_pairs == 1:
            one_expert(weights[0], weights[1])
        else:
            pl.when(step // per == k)(functools.partial(one_expert, weights[2 * k], weights[2 * k + 1]))


def owner_group(ids, picked_x, picked_r, pairs, gate_pad, bufs, first, picks, experts, scale):
    per, cols, width = pairs[0][0].shape
    num = per * len(pairs)
    total = picked_x.shape[0]
    rows = lambda i, ids: (first + i, 0)

    def weight(k):
        return lambda i, ids: (jnp.clip(i - k * per, 0, per - 1), 0, 0)

    in_specs = [pl.BlockSpec((picks, cols), rows), pl.BlockSpec((picks, cols), rows),
                pl.BlockSpec(gate_pad.shape, lambda i, ids: (0, 0))]
    for k in range(len(pairs)):
        in_specs += [pl.BlockSpec((1, cols, width), weight(k)), pl.BlockSpec((1, width, cols), weight(k))]
    alias = {}
    if bufs:
        alias = {1 + len(in_specs) + j: j for j in range(3)}
        in_specs += [pl.BlockSpec(memory_space=pl.ANY)] * 3
    return pl.pallas_call(
        functools.partial(owner_body, first=first, per=per, num_pairs=len(pairs), experts=experts, scale=scale),
        grid_spec=pltpu.PrefetchScalarGridSpec(
            num_scalar_prefetch=1, grid=(num,), in_specs=in_specs,
            out_specs=[pl.BlockSpec((picks, cols), rows), pl.BlockSpec((picks, cols), rows),
                       pl.BlockSpec((picks, LANES), rows)]),
        out_shape=[jax.ShapeDtypeStruct((total, cols), BF16), jax.ShapeDtypeStruct((total, cols), BF16),
                   jax.ShapeDtypeStruct((total, LANES), F32)],
        input_output_aliases=alias,
        compiler_params=pltpu.CompilerParams(dimension_semantics=("arbitrary",), vmem_limit_bytes=48 * MIB),
        cost_estimate=pl.CostEstimate(flops=num * 1_000_000_000, bytes_accessed=num * 4 * MIB, transcendentals=0))(ids, picked_x, picked_r, gate_pad, *[w for pair in pairs for w in pair], *bufs)


def expert_body(ids, x_ref, r_ref, w1_ref, w2_ref, gate_ref, up_ref, down_ref, up_acc, down_acc, *, experts, scale):
    expert = ids[pl.program_id(0)]
    step = pl.program_id(1)
    x_rows = x_ref[...]
    w1, w2 = w1_ref[0], w2_ref[0]
    probs, lane = softmax_rows(x_rows, gate_ref[...], experts)
    gate = jnp.sum(jnp.where(lane == expert, probs, 0.0), axis=1, keepdims=True)
    act, slope = gelu_parts(dot(x_rows, w1))
    dh = (gate * (r_ref[...].astype(F32) * scale)).astype(BF16)
    du = dot_nt(dh, w2).astype(BF16)
    da = (slope * du.astype(F32)).astype(BF16)

    @pl.when(step == 0)
    def _():
        up_acc[...] = jnp.zeros_like(up_acc)
        down_acc[...] = jnp.zeros_like(down_acc)

    down_acc[...] += dot_tn(act.astype(BF16), dh)
    up_acc[...] += dot_tn(x_rows, da)

    @pl.when(step == pl.num_programs(1) - 1)
    def _():
        up_ref[0] = up_acc[...].astype(BF16)
        down_ref[0] = down_acc[...].astype(BF16)


def expert_grads(ids, rows_x, rows_r, w1, w2, gate_pad, experts, scale):
    num, cols, width = w1.shape
    block = 512
    steps = rows_x.shape[0] // num // block
    rows = lambda e, i, ids: (e * steps + i, 0)
    weight = lambda e, i, ids: (e, 0, 0)
    return pl.pallas_call(
        functools.partial(expert_body, experts=experts, scale=scale),
        grid_spec=pltpu.PrefetchScalarGridSpec(
            num_scalar_prefetch=1, grid=(num, steps),
            in_specs=[pl.BlockSpec((block, cols), rows), pl.BlockSpec((block, cols), rows),
                      pl.BlockSpec((1, cols, width), weight), pl.BlockSpec((1, width, cols), weight),
                      pl.BlockSpec(gate_pad.shape, lambda e, i, ids: (0, 0))],
            out_specs=[pl.BlockSpec((1, cols, width), weight), pl.BlockSpec((1, width, cols), weight)],
            scratch_shapes=[pltpu.VMEM((cols, width), F32), pltpu.VMEM((width, cols), F32)]),
        out_shape=[jax.ShapeDtypeStruct(w1.shape, BF16), jax.ShapeDtypeStruct(w2.shape, BF16)],
        compiler_params=pltpu.CompilerParams(dimension_semantics=("arbitrary", "arbitrary"), vmem_limit_bytes=48 * MIB),
        cost_estimate=pl.CostEstimate(flops=45_000_000_000, bytes_accessed=48 * MIB, transcendentals=0),
        name="expert_grads")(ids, rows_x, rows_r, w1, w2, gate_pad)


def add_block(idx, tok, base, h_ref, g_ref, aux_ref, y_acc, g_acc, s_acc, y_stage, g_stage):
    picks = h_ref.shape[0]
    put_rows(y_stage, 0, h_ref[...].astype(F32) * aux_ref[:, 64:65])
    put_rows(g_stage, 0, g_ref[...].astype(F32))
    unroll = 16

    def body(i, carry):
        at = [pl.ds(idx[base + i * unroll + j], 8, stride=8) for j in range(unroll)]
        staged = [pl.ds(i * (unroll * 8) + (j // 8) * 64 + j % 8, 8, stride=8) for j in range(unroll)]
        for acc, stage in ((y_acc, y_stage), (g_acc, g_stage)):
            sums = [acc[at[j], :] + stage[staged[j], :] for j in range(unroll)]
            for j in range(unroll):
                acc[at[j], :] = sums[j]
        row = [pl.ds(tok[base + i * unroll + j], 1) for j in range(unroll)]
        sums = [s_acc[row[j], :] + aux_ref[pl.ds(i * unroll + j, 1), :] for j in range(unroll)]
        for j in range(unroll):
            s_acc[row[j], :] = sums[j]
        return carry

    lax.fori_loop(0, picks // unroll, body, 0)


def start_all(pairs, sem):
    copies = [pltpu.make_async_copy(a, b, sem.at[k]) for k, (a, b) in enumerate(pairs)]
    for copy in copies:
        copy.start()
    return copies


def wait_all(copies):
    for copy in copies:
        copy.wait()


def acc_shapes(tokens):
    return [(tokens * 8, LANES), (tokens * 8, LANES), (tokens, LANES)]


def combine_first_body(idx, tok, x_ref, r_ref, h_ref, g_ref, aux_ref, gate_ref, y_out, g_out, s_out, probs_ref,
                       y_acc, g_acc, s_acc, y_stage, g_stage, sem, *, chunks, blocks, experts, scale):
    step = pl.program_id(0)

    @pl.when(step < chunks)
    def _():
        put_rows(y_acc, step * CHUNK, x_ref[...].astype(F32))
        put_rows(g_acc, step * CHUNK, r_ref[...].astype(F32) * scale)
        s_acc[pl.ds(step * CHUNK, CHUNK), :] = jnp.zeros((CHUNK, LANES), F32)
        probs_ref[...] = softmax_rows(x_ref[...], gate_ref[...], experts)[0]

    @pl.when(step >= chunks)
    def _():
        add_block(idx, tok, (step - chunks) * h_ref.shape[0], h_ref, g_ref, aux_ref, y_acc, g_acc, s_acc, y_stage, g_stage)

    @pl.when(step == chunks + blocks - 1)
    def _():
        wait_all(start_all(((y_acc, y_out), (g_acc, g_out), (s_acc, s_out)), sem))


def combine_first(idx, tok, x, loss_w, h, g, aux, gate_pad, picks, blocks, experts, scale):
    tokens, cols = x.shape
    chunks = tokens // CHUNK
    token_map = lambda i, idx, tok: (jnp.minimum(i, chunks - 1), 0)
    block_map = lambda i, idx, tok: (jnp.maximum(i - chunks, 0), 0)
    return pl.pallas_call(
        functools.partial(combine_first_body, chunks=chunks, blocks=blocks, experts=experts, scale=scale),
        grid_spec=pltpu.PrefetchScalarGridSpec(
            num_scalar_prefetch=2, grid=(chunks + blocks,),
            in_specs=[pl.BlockSpec((CHUNK, cols), token_map), pl.BlockSpec((CHUNK, cols), token_map),
                      pl.BlockSpec((picks, cols), block_map), pl.BlockSpec((picks, cols), block_map),
                      pl.BlockSpec((picks, LANES), block_map), pl.BlockSpec(gate_pad.shape, lambda i, idx, tok: (0, 0))],
            out_specs=[pl.BlockSpec(memory_space=pl.ANY)] * 3 + [pl.BlockSpec((CHUNK, LANES), token_map)],
            scratch_shapes=[pltpu.VMEM(s, F32) for s in acc_shapes(tokens)]
            + [pltpu.VMEM((picks * 8, LANES), F32)] * 2 + [pltpu.SemaphoreType.DMA((3,))]),
        out_shape=[jax.ShapeDtypeStruct(s, F32) for s in acc_shapes(tokens) + [(tokens, LANES)]],
        compiler_params=pltpu.CompilerParams(dimension_semantics=("arbitrary",), vmem_limit_bytes=56 * MIB),
        cost_estimate=pl.CostEstimate(flops=30_000_000_000, bytes_accessed=64 * MIB, transcendentals=0),
        name="combine_first")(idx, tok, x, loss_w, h, g, aux, gate_pad)


def combine_mid_body(idx, tok, h_ref, g_ref, aux_ref, y_in, g_in, s_in, y_out, g_out, s_out,
                     y_acc, g_acc, s_acc, y_stage, g_stage, sem, *, first, blocks):
    step = pl.program_id(0)

    @pl.when(step == 0)
    def _():
        wait_all(start_all(((y_in, y_acc), (g_in, g_acc), (s_in, s_acc)), sem))

    add_block(idx, tok, (first + step) * h_ref.shape[0], h_ref, g_ref, aux_ref, y_acc, g_acc, s_acc, y_stage, g_stage)

    @pl.when(step == blocks - 1)
    def _():
        wait_all(start_all(((y_acc, y_out), (g_acc, g_out), (s_acc, s_out)), sem))


def combine_mid(idx, tok, h, g, aux, accs, picks, first, blocks):
    cols, tokens = h.shape[1], accs[2].shape[0]
    block_map = lambda i, idx, tok: (first + i, 0)
    return pl.pallas_call(
        functools.partial(combine_mid_body, first=first, blocks=blocks),
        grid_spec=pltpu.PrefetchScalarGridSpec(
            num_scalar_prefetch=2, grid=(blocks,),
            in_specs=[pl.BlockSpec((picks, cols), block_map), pl.BlockSpec((picks, cols), block_map),
                      pl.BlockSpec((picks, LANES), block_map)] + [pl.BlockSpec(memory_space=pl.ANY)] * 3,
            out_specs=[pl.BlockSpec(memory_space=pl.ANY)] * 3,
            scratch_shapes=[pltpu.VMEM(s, F32) for s in acc_shapes(tokens)]
            + [pltpu.VMEM((picks * 8, LANES), F32)] * 2 + [pltpu.SemaphoreType.DMA((3,))]),
        out_shape=[jax.ShapeDtypeStruct(s, F32) for s in acc_shapes(tokens)],
        compiler_params=pltpu.CompilerParams(dimension_semantics=("arbitrary",), vmem_limit_bytes=56 * MIB),
        cost_estimate=pl.CostEstimate(flops=20_000_000_000, bytes_accessed=64 * MIB, transcendentals=0),
        name="combine_mid")(idx, tok, h, g, aux, *accs)


DEPTH = 3


def combine_last_body(ids, idx, tok, px_ref, pr_ref, w1_ref, w2_ref, gate_ref, h_ref, g_ref, aux_ref,
                      x_in, r_in, y_in, g_in, s_in, probs_in, y_out, gx_out, part_ref,
                      y_acc, g_acc, s_acc, y_stage, g_stage, h_own, g_own, aux_own, probs, dlogits, sem,
                      x_buf, r_buf, y_buf, gx_buf, in_sem, out_sem,
                      *, own_first, own, first, blocks, experts, scale):
    step = pl.program_id(0)
    picks = h_ref.shape[0]
    loads = ((y_in, y_acc), (g_in, g_acc), (s_in, s_acc), (probs_in, probs))
    state = (y_acc, g_acc, s_acc, y_stage, g_stage)
    rows, cols = x_buf.shape[1:]
    lead = 2 * own + blocks
    passes = x_in.shape[0] // rows

    def fetch(k):
        at, slot = pl.ds(pl.multiple_of(k * rows, rows), rows), lax.rem(k, DEPTH)
        return [pltpu.make_async_copy(x_in.at[at], x_buf.at[slot], in_sem.at[0, slot]),
                pltpu.make_async_copy(r_in.at[at], r_buf.at[slot], in_sem.at[1, slot])]

    def flush(k):
        at, slot = pl.ds(pl.multiple_of(k * rows, rows), rows), lax.rem(k, DEPTH)
        return [pltpu.make_async_copy(y_buf.at[slot], y_out.at[at], out_sem.at[0, slot]),
                pltpu.make_async_copy(gx_buf.at[slot], gx_out.at[at], out_sem.at[1, slot])]

    @pl.when(step == 0)
    def _():
        start_all(loads, sem)

    @pl.when(step < own)
    def _():
        h_own[step], g_own[step], aux_own[step] = owner_expert(
            px_ref[...], pr_ref[...], w1_ref[0], w2_ref[0], gate_ref[...], ids[own_first + step], experts, scale)

    @pl.when(step == own)
    def _():
        wait_all([pltpu.make_async_copy(a, b, sem.at[k]) for k, (a, b) in enumerate(loads)])

    @pl.when((step >= own) & (step < 2 * own))
    def _():
        k = step - own
        add_block(idx, tok, (own_first + k) * picks, h_own.at[k], g_own.at[k], aux_own.at[k], *state)

    @pl.when((step >= 2 * own) & (step < 2 * own + blocks))
    def _():
        add_block(idx, tok, (first + step - 2 * own) * picks, h_ref, g_ref, aux_ref, *state)

    @pl.when(step == lead - 1)
    def _():
        for k in range(DEPTH - 1):
            for copy in fetch(k):
                copy.start()

    def one_pass(k, carry):
        slot = lax.rem(k, DEPTH)
        start = pl.multiple_of(k * rows, rows)

        @pl.when(k + DEPTH - 1 < passes)
        def _():
            for copy in fetch(k + DEPTH - 1):
                copy.start()

        @pl.when(k >= DEPTH)
        def _():
            wait_all(flush(k - DEPTH))

        wait_all(fetch(k))
        dl = dlogits[pl.ds(start, rows), :]
        part_ref[0:experts, :] += dot_tn(dl, x_buf[slot])[0:experts]
        wide = 256
        for c in range(0, cols, wide):
            at = pl.ds(c, wide)
            extra = dot_nt(dl, gate_ref[at, :])
            gx_buf[slot, :, at] = (get_rows(g_acc, start, rows, cols, c, wide) + extra).astype(BF16)
            y = get_rows(y_acc, start, rows, cols, c, wide).astype(BF16)
            y_buf[slot, :, at] = y
            prod = y.astype(F32) * r_buf[slot, :, at].astype(F32)
            part_ref[experts:experts + 8, at] += prod.reshape(rows // 8, 8, wide).sum(axis=0)
        for copy in flush(k):
            copy.start()
        return carry

    @pl.when(step == lead)
    def _():
        part_ref[...] = jnp.zeros_like(part_ref)
        live = lax.broadcasted_iota(jnp.int32, (CHUNK, LANES), 1) < experts

        def softmax_grad(k, carry):
            at = pl.ds(pl.multiple_of(k * CHUNK, CHUNK), CHUNK)
            p = probs[at, :]
            dp = jnp.where(live, s_acc[at, :], 0.0)
            dlogits[at, :] = (p * (dp - jnp.sum(p * dp, axis=1, keepdims=True))).astype(BF16)
            return carry

        lax.fori_loop(0, x_in.shape[0] // CHUNK, softmax_grad, 0)
        lax.fori_loop(0, passes, one_pass, 0)
        for late in range(DEPTH):
            wait_all(flush(passes - DEPTH + late))


def combine_last(ids, idx, tok, x, loss_w, picked_x, picked_r, w1, w2, h, g, aux, gate_pad, accs, probs, picks, first, experts, scale):
    tokens, cols = x.shape
    rows = 256
    own, width = w1.shape[0], w1.shape[2]
    own_first = h.shape[0] // picks - own
    blocks = own_first - first
    lead = 2 * own + blocks
    own_map = lambda i, *_: (own_first + jnp.minimum(i, own - 1), 0)
    weight_map = lambda i, *_: (jnp.minimum(i, own - 1), 0, 0)
    block_map = lambda i, *_: (first + jnp.clip(i - 2 * own, 0, blocks - 1), 0)
    whole = lambda i, *_: (0, 0)
    return pl.pallas_call(
        functools.partial(combine_last_body, own_first=own_first, own=own, first=first, blocks=blocks,
                          experts=experts, scale=scale),
        grid_spec=pltpu.PrefetchScalarGridSpec(
            num_scalar_prefetch=3, grid=(lead + 1,),
            in_specs=[pl.BlockSpec((picks, cols), own_map), pl.BlockSpec((picks, cols), own_map),
                      pl.BlockSpec((1, cols, width), weight_map), pl.BlockSpec((1, width, cols), weight_map),
                      pl.BlockSpec(gate_pad.shape, whole),
                      pl.BlockSpec((picks, cols), block_map), pl.BlockSpec((picks, cols), block_map),
                      pl.BlockSpec((picks, LANES), block_map)]
            + [pl.BlockSpec(memory_space=pl.ANY)] * 6,
            out_specs=[pl.BlockSpec(memory_space=pl.ANY)] * 2 + [pl.BlockSpec((experts + 8, cols), whole)],
            scratch_shapes=[pltpu.VMEM(s, F32) for s in acc_shapes(tokens)]
            + [pltpu.VMEM((picks * 8, LANES), F32)] * 2
            + [pltpu.VMEM((own, picks, cols), BF16)] * 2 + [pltpu.VMEM((own, picks, LANES), F32)]
            + [pltpu.VMEM((tokens, LANES), F32), pltpu.VMEM((tokens, LANES), BF16)]
            + [pltpu.SemaphoreType.DMA((4,))] + [pltpu.VMEM((DEPTH, rows, cols), BF16)] * 4
            + [pltpu.SemaphoreType.DMA((2, DEPTH))] * 2),
        out_shape=[jax.ShapeDtypeStruct(x.shape, BF16), jax.ShapeDtypeStruct(x.shape, BF16),
                   jax.ShapeDtypeStruct((experts + 8, cols), F32)],
        compiler_params=pltpu.CompilerParams(dimension_semantics=("arbitrary",), vmem_limit_bytes=60 * MIB),
        cost_estimate=pl.CostEstimate(flops=50_000_000_000, bytes_accessed=64 * MIB, transcendentals=0),
        name="combine_last")(ids, idx, tok, picked_x, picked_r, w1, w2, gate_pad, h, g, aux, x, loss_w, *accs, probs)


def rank_picks(tok, tokens, distinct):
    side = 64
    steps = jnp.arange(side)
    hi = (tok // side)[..., None] == steps
    lo = (tok % side)[..., None] == steps
    hist = jnp.einsum('tph,tpl->thl', hi.astype(BF16), lo.astype(BF16), preferred_element_type=F32)
    seen = (hist > 0).astype(BF16)
    upto = (steps[:, None] <= steps[None, :]).astype(BF16)
    within = jnp.einsum('thl,lk->thk', seen, upto, preferred_element_type=F32)
    before = jnp.sum(jnp.where(steps[None, :, None] > steps[None, None, :], within[:, None, :, -1], 0.0), axis=-1)
    count = within + before[..., None]
    row = jnp.einsum('tph,thl->tpl', hi.astype(BF16), within.astype(BF16), preferred_element_type=F32)
    start = jnp.sum(jnp.where(hi, before[:, None, :], 0.0), axis=-1)
    place = (jnp.sum(jnp.where(lo, row, 0.0), axis=-1) + start - 1.0).astype(jnp.int32)
    flat = count.reshape(tok.shape[0], 1, tokens)
    listed = jnp.sum((flat <= jnp.arange(distinct, dtype=F32)[None, :, None]).astype(jnp.int32), axis=-1)
    return listed, place


def after(value, *earlier):
    return lax.optimization_barrier((value, *earlier))[0]


def solution(mesh):
    group = mesh.shape['ep']

    def permute(value, mask):
        return lax.ppermute(value, 'ep', [(i, i ^ mask) for i in range(group)])

    def dispatch(rows):
        size = rows.shape[0] // group
        return [rows[:size]] + [permute(rows[m * size:(m + 1) * size], m) for m in range(1, group)]

    def device_step(x, gate_w, up_w, down_w, expert_picks, loss_w):
        tokens, cols = x.shape
        experts = gate_w.shape[1]
        local, capacity = expert_picks.shape
        picks = capacity // group
        distinct = local * picks // 2
        scale = 1.0 / math.sqrt(tokens * group * cols)
        me = lax.axis_index('ep')
        order = me ^ jnp.arange(group)
        gate_pad = jnp.pad(gate_w, ((0, 0), (0, LANES - experts)))

        wanted = expert_picks.reshape(local, group, picks)
        asked = lax.all_to_all(wanted, 'ep', 1, 1, tiled=True) - me * tokens
        asked = jnp.take(asked, order, axis=1).transpose(1, 0, 2)
        wanted = (jnp.take(wanted, order, axis=1) - (order * tokens)[None, :, None]).transpose(1, 0, 2)

        half = local // 2
        part_a = (up_w[:half], down_w[:half])
        xa, ya = [permute(v, 2) for v in part_a], [permute(v, 4) for v in part_a]
        partner = [permute(up_w, 1), permute(down_w, 1)]

        send_list, _ = rank_picks(asked.reshape(group, -1), tokens, distinct)
        send_idx = row_base(send_list).reshape(-1)
        send_x = gather_rows(send_idx, [x], group * distinct)
        send_r = gather_rows(after(send_idx, send_x), [loss_w], group * distinct)
        got_x, got_r = dispatch(send_x), dispatch(send_r)

        part_b = [w[half:] for w in after((up_w, down_w), send_r)]
        xb, yb = [permute(v, 2) for v in part_b], [permute(v, 4) for v in part_b]

        spans = [(0, 0, local), (1, 0, local)] + [(m, 0, half) for m in (2, 4, 3, 5)]
        early = sum(s[2] for s in spans)
        spans += [(m, half, half) for m in (2, 4, 3, 5)] + [(6, 0, half), (7, 0, half), (6, half, half), (7, half, half)]
        ids_by_mask = order[:, None] * local + jnp.arange(local)[None, :]
        own_ids = jnp.concatenate([ids_by_mask[m, s:s + n] for m, s, n in spans])
        own_tok = jnp.concatenate([asked[m, s:s + n] for m, s, n in spans]).reshape(-1)
        own_idx = row_base(own_tok)
        picked_x = gather_rows(after(own_idx, send_r), [x], experts * picks)
        picked_r = gather_rows(after(own_idx, picked_x), [loss_w], experts * picks)

        def relay(vx, vy):
            return [permute(vx[0], 4), permute(vy[1], 2)]

        da, db = relay(xa, ya), relay(xb, yb)
        xa1, ya1, xb1, yb1, da1, db1 = ([permute(v, 1) for v in vs] for vs in (xa, ya, xb, yb, da, db))

        def owner(bufs, first, *pairs):
            ids = after(own_ids, bufs[2]) if bufs else own_ids
            return owner_group(ids, picked_x, picked_r, pairs, gate_pad, bufs, first, picks, experts, scale)

        bufs = owner([], 0, (up_w, down_w))
        bufs = owner(bufs, local, partner)
        bufs = owner(bufs, 2 * local, xa, ya, xa1, ya1)

        _, place = rank_picks(wanted.reshape(group, -1), tokens, distinct)
        rows_idx = row_base(place.reshape(group, local, picks) + jnp.arange(group)[:, None, None] * distinct)
        rows_idx = rows_idx.transpose(1, 0, 2).reshape(-1)
        my_ids = me * local + jnp.arange(local)
        rows_x = gather_rows(after(rows_idx, bufs[2]), got_x, local * capacity)
        *accs, probs = combine_first(after(own_idx, rows_x), own_tok, x, loss_w, *bufs, gate_pad, picks, early, experts, scale)
        rows_r = gather_rows(after(rows_idx, accs[2]), got_r, local * capacity)
        grad_up, grad_down = expert_grads(my_ids, rows_x, rows_r, up_w, down_w, gate_pad, experts, scale)

        own_ids = after(own_ids, grad_down)
        bufs = owner(bufs, 4 * local, xb, yb)
        bufs = owner(bufs, 5 * local, xb1, yb1)
        accs = combine_mid(own_idx, own_tok, *bufs, accs, picks, early, 2 * local)
        own_ids = after(own_ids, accs[2])
        bufs = owner(bufs, 6 * local, da)
        bufs = owner(bufs, 6 * local + half, da1)
        bufs = owner(bufs, 7 * local, db)
        y, grad_x, part = combine_last(own_ids, own_idx, own_tok, x, loss_w, picked_x, picked_r, *db1, *bufs, gate_pad,
                                       accs, probs, picks, 6 * local, experts, scale)
        part = part + permute(part, 1)
        part = (part + permute(part, 2)) + (permute(part, 4) + permute(part, 6))
        return y, jnp.sum(part[experts:]) * scale, grad_x, grad_up, grad_down, part[:experts].T

    return jax.shard_map(device_step, mesh=mesh,
                         in_specs=(P('ep'), P(), P('ep'), P('ep'), P('ep'), P('ep')),
                         out_specs=(P('ep'), P(), P('ep'), P('ep'), P('ep'), P()),
                         check_vma=False)
```

```python
import functools
import math
import jax
import jax.numpy as jnp
from jax import lax
from jax.experimental import pallas as pl
from jax.experimental.pallas import tpu as pltpu
from jax.sharding import PartitionSpec as P


F32, BF16 = jnp.float32, jnp.bfloat16
LANES = 128
CHUNK = 512
MIB = 2**20
GRANT = 60 * MIB
WEIGHTS = 3


def as_tiles(ref, cols):
    return ref.reshape(ref.shape[0] * LANES // (8 * cols), cols // LANES, 8, LANES)


def put_rows(ref, start, value):
    rows, cols = value.shape
    tiles = as_tiles(ref, cols)
    for c in range(cols // LANES):
        tiles[pl.ds(start // 8, rows // 8), c] = value[:, c * LANES:(c + 1) * LANES].reshape(rows // 8, 8, LANES)


def get_rows(ref, start, rows, cols, first=0, wide=None):
    tiles = as_tiles(ref, cols)
    spans = range(first // LANES, (first + (wide or cols)) // LANES)
    return jnp.concatenate([tiles[pl.ds(start // 8, rows // 8), c].reshape(rows, LANES) for c in spans], axis=1)


def row_base(row):
    return ((row >> 3) << 6) | (row & 7)


def gather_body(idx, *refs, num_src, rows, block, split):
    srcs, outs = refs[:num_src], refs[num_src:num_src + split + 1]
    src32, stage, buf, sem = refs[num_src + split + 1:num_src + split + 5]
    step = pl.program_id(0)
    chunks = rows // CHUNK

    @pl.when(step == 0)
    def _():
        def load(src, k):
            return pltpu.make_async_copy(src, buf.at[k % 2], sem.at[k % 2])

        def start(k):
            if num_src == 1:
                load(srcs[0].at[pl.ds(pl.multiple_of(k * CHUNK, CHUNK), CHUNK)], k).start()
            for i in range(num_src if num_src > 1 else 0):
                pl.when(k == i)(lambda i=i: load(srcs[i], i).start())

        def convert(k, carry):
            pl.when(k + 1 < chunks)(lambda: start(k + 1))
            load(srcs[0].at[pl.ds(0, CHUNK)], k).wait()
            put_rows(src32, k * CHUNK, buf[k % 2].astype(F32))
            return carry

        start(jnp.int32(0))
        lax.fori_loop(0, chunks, convert, 0)

    unroll = 16

    def body(i, carry):
        vals = [src32[pl.ds(idx[step * block + i * unroll + j], 8, stride=8), :] for j in range(unroll)]
        for j in range(unroll):
            stage[pl.ds(i * (unroll * 8) + (j // 8) * 64 + j % 8, 8, stride=8), :] = vals[j]
        return carry

    lax.fori_loop(0, block // unroll, body, 0)
    cols = srcs[0].shape[1]
    if not split:
        outs[0][...] = get_rows(stage, 0, block, cols).astype(BF16)
        return

    out_buf, out_sem = refs[-2:]
    slot = lax.rem(step, 2)

    def save(dst, at):
        return pltpu.make_async_copy(out_buf.at[at], dst, out_sem.at[at])

    first_rows = outs[-1].at[pl.ds(0, block)]
    pl.when(step >= 2)(lambda: save(first_rows, slot).wait())
    out_buf[slot] = get_rows(stage, 0, block, cols).astype(BF16)
    for i in range(split):
        pl.when(step == i)(lambda i=i: save(outs[i], slot).start())

    @pl.when(step >= split)
    def _():
        save(outs[-1].at[pl.ds(pl.multiple_of((step - split) * block, block), block)], slot).start()

    @pl.when(step == pl.num_programs(0) - 1)
    def _():
        save(first_rows, 1 - slot).wait()
        save(first_rows, slot).wait()


def gather_rows(idx, srcs, num_out, split=0):
    rows, cols = sum(s.shape[0] for s in srcs), srcs[0].shape[1]
    block = 512
    scratch = [pltpu.VMEM((rows * 8, LANES), F32), pltpu.VMEM((block * 8, LANES), F32),
               pltpu.VMEM((2, CHUNK, cols), BF16), pltpu.SemaphoreType.DMA((2,))]
    out_specs = pl.BlockSpec((block, cols), lambda i, idx: (i, 0))
    out_shape = jax.ShapeDtypeStruct((num_out, cols), BF16)
    if split:
        scratch += [pltpu.VMEM((2, block, cols), BF16), pltpu.SemaphoreType.DMA((2,))]
        out_specs = [pl.BlockSpec(memory_space=pl.ANY)] * (split + 1)
        out_shape = [jax.ShapeDtypeStruct((block, cols), BF16)] * split + [jax.ShapeDtypeStruct((num_out - split * block, cols), BF16)]
    return pl.pallas_call(
        functools.partial(gather_body, num_src=len(srcs), rows=rows, block=block, split=split),
        grid_spec=pltpu.PrefetchScalarGridSpec(
            num_scalar_prefetch=1, grid=(num_out // block,),
            in_specs=[pl.BlockSpec(memory_space=pl.ANY)] * len(srcs), out_specs=out_specs, scratch_shapes=scratch),
        out_shape=out_shape,
        compiler_params=pltpu.CompilerParams(dimension_semantics=("arbitrary",), vmem_limit_bytes=GRANT),
        cost_estimate=pl.CostEstimate(flops=num_out * 1_000_000, bytes_accessed=num_out * cols * 4, transcendentals=0))(idx, *srcs)


def dot(a, b):
    return lax.dot_general(a, b, (((1,), (0,)), ((), ())), preferred_element_type=F32)


def dot_nt(a, b):
    return lax.dot_general(a, b, (((1,), (1,)), ((), ())), preferred_element_type=F32)


def dot_tn(a, b):
    return lax.dot_general(a, b, (((0,), (0,)), ((), ())), preferred_element_type=F32)


def softmax_rows(x_rows, gate_pad, experts):
    logits = dot(x_rows, gate_pad)
    lane = lax.broadcasted_iota(jnp.int32, logits.shape, 1)
    live = lane < experts
    logits = jnp.where(live, logits, -jnp.inf)
    e = jnp.exp(logits - jnp.max(logits, axis=1, keepdims=True))
    return e / jnp.sum(e, axis=1, keepdims=True), lane


def gelu_parts(a):
    c = math.sqrt(2.0 / math.pi)
    sq = a * a
    t = jnp.tanh(c * (a + 0.044715 * (sq * a)))
    half = 0.5 * (1.0 + t)
    return a * half, half + (0.5 * a) * (1.0 - t * t) * (c + (3.0 * 0.044715 * c) * sq)


def owner_expert(x_rows, r_rows, w1, w2, gate_pad, expert, experts, scale):
    probs, lane = softmax_rows(x_rows, gate_pad, experts)
    gate = jnp.sum(jnp.where(lane == expert, probs, 0.0), axis=1, keepdims=True)
    act, slope = gelu_parts(dot(x_rows, w1))
    h = dot(act.astype(BF16), w2).astype(BF16)
    dy = r_rows.astype(F32) * scale
    gate_grad = jnp.sum(dy * h.astype(F32), axis=1, keepdims=True)
    dh = (gate * dy).astype(BF16)
    du = dot_nt(dh, w2).astype(BF16)
    da = (slope * du.astype(F32)).astype(BF16)
    aux = jnp.where(lane == expert, gate_grad, jnp.where(lane == 64, gate, 0.0))
    return h, dot_nt(da, w1).astype(BF16), aux


def owner_body(ids, x_ref, r_ref, gate_ref, *refs, first, per, num_pairs, experts, scale):
    weights = refs[:2 * num_pairs]
    step = pl.program_id(0)
    if num_pairs == 1:
        h_ref, g_ref, aux_ref = refs[-3:]
        h_ref[...], g_ref[...], aux_ref[...] = owner_expert(
            x_ref[...], r_ref[...], weights[0][0], weights[1][0], gate_ref[...], ids[first + step], experts, scale)
        return
    h_ref, g_ref, aux_ref, w1_buf, w2_buf, sem = refs[-6:]
    num = per * num_pairs

    def load(w1, w2, at, i):
        slot = lax.rem(i, WEIGHTS)
        return [pltpu.make_async_copy(w1.at[at], w1_buf.at[slot], sem.at[0, slot]),
                pltpu.make_async_copy(w2.at[at], w2_buf.at[slot], sem.at[1, slot])]

    def start(i):
        for k in range(num_pairs):
            @pl.when((i >= k * per) & (i < (k + 1) * per))
            def _():
                start_all(load(weights[2 * k], weights[2 * k + 1], i - k * per, i))

    @pl.when(step == 0)
    def _():
        for i in range(min(WEIGHTS - 1, num)):
            start(jnp.int32(i))

    start(step + WEIGHTS - 1)
    wait_all(load(weights[0], weights[1], 0, step))
    slot = lax.rem(step, WEIGHTS)
    h_ref[...], g_ref[...], aux_ref[...] = owner_expert(
        x_ref[...], r_ref[...], w1_buf[slot], w2_buf[slot], gate_ref[...], ids[first + step], experts, scale)


def owner_group(ids, picked_x, picked_r, pairs, gate_pad, bufs, first, picks, experts, scale):
    per, cols, width = pairs[0][0].shape
    num = per * len(pairs)
    total = picked_x.shape[0]
    rows = lambda i, ids: (first + i, 0)
    in_specs = [pl.BlockSpec((picks, cols), rows), pl.BlockSpec((picks, cols), rows),
                pl.BlockSpec(gate_pad.shape, lambda i, ids: (0, 0))]
    scratch = []
    if len(pairs) == 1:
        weight = lambda i, ids: (i, 0, 0)
        in_specs += [pl.BlockSpec((1, cols, width), weight), pl.BlockSpec((1, width, cols), weight)]
    else:
        in_specs += [pl.BlockSpec(memory_space=pl.ANY)] * (2 * len(pairs))
        scratch = [pltpu.VMEM((WEIGHTS, cols, width), BF16), pltpu.VMEM((WEIGHTS, width, cols), BF16),
                   pltpu.SemaphoreType.DMA((2, WEIGHTS))]
    alias = {}
    if bufs:
        alias = {1 + len(in_specs) + j: j for j in range(3)}
        in_specs += [pl.BlockSpec(memory_space=pl.ANY)] * 3
    return pl.pallas_call(
        functools.partial(owner_body, first=first, per=per, num_pairs=len(pairs), experts=experts, scale=scale),
        grid_spec=pltpu.PrefetchScalarGridSpec(
            num_scalar_prefetch=1, grid=(num,), in_specs=in_specs,
            out_specs=[pl.BlockSpec((picks, cols), rows), pl.BlockSpec((picks, cols), rows),
                       pl.BlockSpec((picks, LANES), rows)],
            scratch_shapes=scratch),
        out_shape=[jax.ShapeDtypeStruct((total, cols), BF16), jax.ShapeDtypeStruct((total, cols), BF16),
                   jax.ShapeDtypeStruct((total, LANES), F32)],
        input_output_aliases=alias,
        compiler_params=pltpu.CompilerParams(dimension_semantics=("arbitrary",), vmem_limit_bytes=GRANT),
        cost_estimate=pl.CostEstimate(flops=num * 1_000_000_000, bytes_accessed=num * 4 * MIB, transcendentals=0))(ids, picked_x, picked_r, gate_pad, *[w for pair in pairs for w in pair], *bufs)


def expert_body(ids, x_ref, r_ref, w1_ref, w2_ref, gate_ref, *refs, carried, experts, scale):
    up_ref, down_ref, up_acc, down_acc = refs[-4:]
    expert = ids[pl.program_id(0)]
    step = pl.program_id(1)
    x_rows = x_ref[...]
    w1, w2 = w1_ref[0], w2_ref[0]
    probs, lane = softmax_rows(x_rows, gate_ref[...], experts)
    gate = jnp.sum(jnp.where(lane == expert, probs, 0.0), axis=1, keepdims=True)
    act, slope = gelu_parts(dot(x_rows, w1))
    dh = (gate * (r_ref[...].astype(F32) * scale)).astype(BF16)
    du = dot_nt(dh, w2).astype(BF16)
    da = (slope * du.astype(F32)).astype(BF16)

    @pl.when(step == 0)
    def _():
        if carried:
            up_acc[...] = refs[0][0]
            down_acc[...] = refs[1][0]
        else:
            up_acc[...] = jnp.zeros_like(up_acc)
            down_acc[...] = jnp.zeros_like(down_acc)

    down_acc[...] += dot_tn(act.astype(BF16), dh)
    up_acc[...] += dot_tn(x_rows, da)

    @pl.when(step == pl.num_programs(1) - 1)
    def _():
        up_ref[0] = up_acc[...].astype(up_ref.dtype)
        down_ref[0] = down_acc[...].astype(down_ref.dtype)


def expert_grads(ids, rows_x, first_x, rows_r, w1, w2, gate_pad, sums, out_type, experts, scale):
    num, cols, width = w1.shape
    block = 512
    steps = rows_r.shape[0] // num // block
    skip = first_x // block
    weight = lambda e, i, ids: (e, 0, 0)
    grads = [pl.BlockSpec((1, cols, width), weight), pl.BlockSpec((1, width, cols), weight)]
    return pl.pallas_call(
        functools.partial(expert_body, carried=bool(sums), experts=experts, scale=scale),
        grid_spec=pltpu.PrefetchScalarGridSpec(
            num_scalar_prefetch=1, grid=(num, steps),
            in_specs=[pl.BlockSpec((block, cols), lambda e, i, ids: (skip + e * steps + i, 0)),
                      pl.BlockSpec((block, cols), lambda e, i, ids: (e * steps + i, 0)),
                      pl.BlockSpec((1, cols, width), weight), pl.BlockSpec((1, width, cols), weight),
                      pl.BlockSpec(gate_pad.shape, lambda e, i, ids: (0, 0))] + (grads if sums else []),
            out_specs=grads,
            scratch_shapes=[pltpu.VMEM((cols, width), F32), pltpu.VMEM((width, cols), F32)]),
        out_shape=[jax.ShapeDtypeStruct(w1.shape, out_type), jax.ShapeDtypeStruct(w2.shape, out_type)],
        compiler_params=pltpu.CompilerParams(dimension_semantics=("arbitrary", "arbitrary"), vmem_limit_bytes=GRANT),
        cost_estimate=pl.CostEstimate(flops=num * steps * 3_000_000_000, bytes_accessed=48 * MIB, transcendentals=0))(ids, rows_x, rows_r, w1, w2, gate_pad, *sums)


def add_block(idx, tok, base, h_ref, g_ref, aux_ref, y_acc, g_acc, s_acc, y_stage, g_stage):
    picks = h_ref.shape[0]
    put_rows(y_stage, 0, h_ref[...].astype(F32) * aux_ref[:, 64:65])
    put_rows(g_stage, 0, g_ref[...].astype(F32))
    unroll = 16

    def body(i, carry):
        at = [pl.ds(idx[base + i * unroll + j], 8, stride=8) for j in range(unroll)]
        staged = [pl.ds(i * (unroll * 8) + (j // 8) * 64 + j % 8, 8, stride=8) for j in range(unroll)]
        for acc, stage in ((y_acc, y_stage), (g_acc, g_stage)):
            sums = [acc[at[j], :] + stage[staged[j], :] for j in range(unroll)]
            for j in range(unroll):
                acc[at[j], :] = sums[j]
        row = [pl.ds(tok[base + i * unroll + j], 1) for j in range(unroll)]
        sums = [s_acc[row[j], :] + aux_ref[pl.ds(i * unroll + j, 1), :] for j in range(unroll)]
        for j in range(unroll):
            s_acc[row[j], :] = sums[j]
        return carry

    lax.fori_loop(0, picks // unroll, body, 0)


def start_pairs(pairs, sem):
    copies = [pltpu.make_async_copy(a, b, sem.at[k]) for k, (a, b) in enumerate(pairs)]
    start_all(copies)
    return copies


def start_all(copies):
    for copy in copies:
        copy.start()


def wait_all(copies):
    for copy in copies:
        copy.wait()


def acc_shapes(tokens):
    return [(tokens * 8, LANES), (tokens * 8, LANES), (tokens, LANES)]


def combine_first_body(idx, tok, x_ref, r_ref, h_ref, g_ref, aux_ref, gate_ref, y_out, g_out, s_out, probs_ref,
                       y_acc, g_acc, s_acc, y_stage, g_stage, sem, *, chunks, blocks, experts, scale):
    step = pl.program_id(0)

    @pl.when(step < chunks)
    def _():
        put_rows(y_acc, step * CHUNK, x_ref[...].astype(F32))
        put_rows(g_acc, step * CHUNK, r_ref[...].astype(F32) * scale)
        s_acc[pl.ds(step * CHUNK, CHUNK), :] = jnp.zeros((CHUNK, LANES), F32)
        probs_ref[...] = softmax_rows(x_ref[...], gate_ref[...], experts)[0]

    @pl.when(step >= chunks)
    def _():
        add_block(idx, tok, (step - chunks) * h_ref.shape[0], h_ref, g_ref, aux_ref, y_acc, g_acc, s_acc, y_stage, g_stage)

    @pl.when(step == chunks + blocks - 1)
    def _():
        wait_all(start_pairs(((y_acc, y_out), (g_acc, g_out), (s_acc, s_out)), sem))


def combine_first(idx, tok, x, loss_w, h, g, aux, gate_pad, picks, blocks, experts, scale):
    tokens, cols = x.shape
    chunks = tokens // CHUNK
    token_map = lambda i, idx, tok: (jnp.minimum(i, chunks - 1), 0)
    block_map = lambda i, idx, tok: (jnp.maximum(i - chunks, 0), 0)
    return pl.pallas_call(
        functools.partial(combine_first_body, chunks=chunks, blocks=blocks, experts=experts, scale=scale),
        grid_spec=pltpu.PrefetchScalarGridSpec(
            num_scalar_prefetch=2, grid=(chunks + blocks,),
            in_specs=[pl.BlockSpec((CHUNK, cols), token_map), pl.BlockSpec((CHUNK, cols), token_map),
                      pl.BlockSpec((picks, cols), block_map), pl.BlockSpec((picks, cols), block_map),
                      pl.BlockSpec((picks, LANES), block_map), pl.BlockSpec(gate_pad.shape, lambda i, idx, tok: (0, 0))],
            out_specs=[pl.BlockSpec(memory_space=pl.ANY)] * 3 + [pl.BlockSpec((CHUNK, LANES), token_map)],
            scratch_shapes=[pltpu.VMEM(s, F32) for s in acc_shapes(tokens)]
            + [pltpu.VMEM((picks * 8, LANES), F32)] * 2 + [pltpu.SemaphoreType.DMA((3,))]),
        out_shape=[jax.ShapeDtypeStruct(s, F32) for s in acc_shapes(tokens) + [(tokens, LANES)]],
        compiler_params=pltpu.CompilerParams(dimension_semantics=("arbitrary",), vmem_limit_bytes=GRANT),
        cost_estimate=pl.CostEstimate(flops=30_000_000_000, bytes_accessed=64 * MIB, transcendentals=0),
        name="combine_first")(idx, tok, x, loss_w, h, g, aux, gate_pad)


def combine_mid_body(idx, tok, h_ref, g_ref, aux_ref, y_in, g_in, s_in, y_out, g_out, s_out,
                     y_acc, g_acc, s_acc, y_stage, g_stage, sem, *, first, blocks):
    step = pl.program_id(0)

    @pl.when(step == 0)
    def _():
        wait_all(start_pairs(((y_in, y_acc), (g_in, g_acc), (s_in, s_acc)), sem))

    add_block(idx, tok, (first + step) * h_ref.shape[0], h_ref, g_ref, aux_ref, y_acc, g_acc, s_acc, y_stage, g_stage)

    @pl.when(step == blocks - 1)
    def _():
        wait_all(start_pairs(((y_acc, y_out), (g_acc, g_out), (s_acc, s_out)), sem))


def combine_mid(idx, tok, h, g, aux, accs, picks, first, blocks):
    cols, tokens = h.shape[1], accs[2].shape[0]
    block_map = lambda i, idx, tok: (first + i, 0)
    return pl.pallas_call(
        functools.partial(combine_mid_body, first=first, blocks=blocks),
        grid_spec=pltpu.PrefetchScalarGridSpec(
            num_scalar_prefetch=2, grid=(blocks,),
            in_specs=[pl.BlockSpec((picks, cols), block_map), pl.BlockSpec((picks, cols), block_map),
                      pl.BlockSpec((picks, LANES), block_map)] + [pl.BlockSpec(memory_space=pl.ANY)] * 3,
            out_specs=[pl.BlockSpec(memory_space=pl.ANY)] * 3,
            scratch_shapes=[pltpu.VMEM(s, F32) for s in acc_shapes(tokens)]
            + [pltpu.VMEM((picks * 8, LANES), F32)] * 2 + [pltpu.SemaphoreType.DMA((3,))]),
        out_shape=[jax.ShapeDtypeStruct(s, F32) for s in acc_shapes(tokens)],
        compiler_params=pltpu.CompilerParams(dimension_semantics=("arbitrary",), vmem_limit_bytes=GRANT),
        cost_estimate=pl.CostEstimate(flops=20_000_000_000, bytes_accessed=64 * MIB, transcendentals=0),
        name="combine_mid")(idx, tok, h, g, aux, *accs)


DEPTH = 3


def combine_last_body(ids, idx, tok, px_ref, pr_ref, w1_ref, w2_ref, gate_ref, h_ref, g_ref, aux_ref,
                      x_in, r_in, y_in, g_in, s_in, probs_in, y_out, gx_out, part_ref,
                      y_acc, g_acc, s_acc, y_stage, g_stage, h_own, g_own, aux_own, probs, dlogits, sem,
                      x_buf, r_buf, y_buf, gx_buf, in_sem, out_sem,
                      *, own_first, own, first, blocks, experts, scale):
    step = pl.program_id(0)
    picks = h_ref.shape[0]
    loads = ((y_in, y_acc), (g_in, g_acc), (s_in, s_acc), (probs_in, probs))
    state = (y_acc, g_acc, s_acc, y_stage, g_stage)
    rows, cols = x_buf.shape[1:]
    lead = 2 * own + blocks
    passes = x_in.shape[0] // rows

    def fetch(k):
        at, slot = pl.ds(pl.multiple_of(k * rows, rows), rows), lax.rem(k, DEPTH)
        return [pltpu.make_async_copy(x_in.at[at], x_buf.at[slot], in_sem.at[0, slot]),
                pltpu.make_async_copy(r_in.at[at], r_buf.at[slot], in_sem.at[1, slot])]

    def flush(k):
        at, slot = pl.ds(pl.multiple_of(k * rows, rows), rows), lax.rem(k, DEPTH)
        return [pltpu.make_async_copy(y_buf.at[slot], y_out.at[at], out_sem.at[0, slot]),
                pltpu.make_async_copy(gx_buf.at[slot], gx_out.at[at], out_sem.at[1, slot])]

    @pl.when(step == 0)
    def _():
        start_pairs(loads, sem)

    @pl.when(step < own)
    def _():
        h_own[step], g_own[step], aux_own[step] = owner_expert(
            px_ref[...], pr_ref[...], w1_ref[0], w2_ref[0], gate_ref[...], ids[own_first + step], experts, scale)

    @pl.when(step == own)
    def _():
        wait_all([pltpu.make_async_copy(a, b, sem.at[k]) for k, (a, b) in enumerate(loads)])

    @pl.when((step >= own) & (step < 2 * own))
    def _():
        k = step - own
        add_block(idx, tok, (own_first + k) * picks, h_own.at[k], g_own.at[k], aux_own.at[k], *state)

    @pl.when((step >= 2 * own) & (step < 2 * own + blocks))
    def _():
        add_block(idx, tok, (first + step - 2 * own) * picks, h_ref, g_ref, aux_ref, *state)

    @pl.when(step == lead - 1)
    def _():
        for k in range(DEPTH - 1):
            for copy in fetch(k):
                copy.start()

    def one_pass(k, carry):
        slot = lax.rem(k, DEPTH)
        start = pl.multiple_of(k * rows, rows)

        @pl.when(k + DEPTH - 1 < passes)
        def _():
            for copy in fetch(k + DEPTH - 1):
                copy.start()

        @pl.when(k >= DEPTH)
        def _():
            wait_all(flush(k - DEPTH))

        wait_all(fetch(k))
        dl = dlogits[pl.ds(start, rows), :]
        part_ref[0:experts, :] += dot_tn(dl, x_buf[slot])[0:experts]
        wide = 256
        for c in range(0, cols, wide):
            at = pl.ds(c, wide)
            extra = dot_nt(dl, gate_ref[at, :])
            gx_buf[slot, :, at] = (get_rows(g_acc, start, rows, cols, c, wide) + extra).astype(BF16)
            y = get_rows(y_acc, start, rows, cols, c, wide).astype(BF16)
            y_buf[slot, :, at] = y
            prod = y.astype(F32) * r_buf[slot, :, at].astype(F32)
            part_ref[experts:experts + 8, at] += prod.reshape(rows // 8, 8, wide).sum(axis=0)
        for copy in flush(k):
            copy.start()
        return carry

    @pl.when(step == lead)
    def _():
        part_ref[...] = jnp.zeros_like(part_ref)
        live = lax.broadcasted_iota(jnp.int32, (CHUNK, LANES), 1) < experts

        def softmax_grad(k, carry):
            at = pl.ds(pl.multiple_of(k * CHUNK, CHUNK), CHUNK)
            p = probs[at, :]
            dp = jnp.where(live, s_acc[at, :], 0.0)
            dlogits[at, :] = (p * (dp - jnp.sum(p * dp, axis=1, keepdims=True))).astype(BF16)
            return carry

        lax.fori_loop(0, x_in.shape[0] // CHUNK, softmax_grad, 0)
        lax.fori_loop(0, passes, one_pass, 0)
        for late in range(DEPTH):
            wait_all(flush(passes - DEPTH + late))


def combine_last(ids, idx, tok, x, loss_w, picked_x, picked_r, w1, w2, h, g, aux, gate_pad, accs, probs, picks, first, experts, scale):
    tokens, cols = x.shape
    rows = 256
    own, width = w1.shape[0], w1.shape[2]
    own_first = h.shape[0] // picks - own
    blocks = own_first - first
    lead = 2 * own + blocks
    own_map = lambda i, *_: (own_first + jnp.minimum(i, own - 1), 0)
    weight_map = lambda i, *_: (jnp.minimum(i, own - 1), 0, 0)
    block_map = lambda i, *_: (first + jnp.clip(i - 2 * own, 0, blocks - 1), 0)
    whole = lambda i, *_: (0, 0)
    return pl.pallas_call(
        functools.partial(combine_last_body, own_first=own_first, own=own, first=first, blocks=blocks,
                          experts=experts, scale=scale),
        grid_spec=pltpu.PrefetchScalarGridSpec(
            num_scalar_prefetch=3, grid=(lead + 1,),
            in_specs=[pl.BlockSpec((picks, cols), own_map), pl.BlockSpec((picks, cols), own_map),
                      pl.BlockSpec((1, cols, width), weight_map), pl.BlockSpec((1, width, cols), weight_map),
                      pl.BlockSpec(gate_pad.shape, whole),
                      pl.BlockSpec((picks, cols), block_map), pl.BlockSpec((picks, cols), block_map),
                      pl.BlockSpec((picks, LANES), block_map)]
            + [pl.BlockSpec(memory_space=pl.ANY)] * 6,
            out_specs=[pl.BlockSpec(memory_space=pl.ANY)] * 2 + [pl.BlockSpec((experts + 8, cols), whole)],
            scratch_shapes=[pltpu.VMEM(s, F32) for s in acc_shapes(tokens)]
            + [pltpu.VMEM((picks * 8, LANES), F32)] * 2
            + [pltpu.VMEM((own, picks, cols), BF16)] * 2 + [pltpu.VMEM((own, picks, LANES), F32)]
            + [pltpu.VMEM((tokens, LANES), F32), pltpu.VMEM((tokens, LANES), BF16)]
            + [pltpu.SemaphoreType.DMA((4,))] + [pltpu.VMEM((DEPTH, rows, cols), BF16)] * 4
            + [pltpu.SemaphoreType.DMA((2, DEPTH))] * 2),
        out_shape=[jax.ShapeDtypeStruct(x.shape, BF16), jax.ShapeDtypeStruct(x.shape, BF16),
                   jax.ShapeDtypeStruct((experts + 8, cols), F32)],
        compiler_params=pltpu.CompilerParams(dimension_semantics=("arbitrary",), vmem_limit_bytes=GRANT),
        cost_estimate=pl.CostEstimate(flops=50_000_000_000, bytes_accessed=64 * MIB, transcendentals=0),
        name="combine_last")(ids, idx, tok, picked_x, picked_r, w1, w2, gate_pad, h, g, aux, x, loss_w, *accs, probs)


def rank_picks(tok, distinct):
    side = 64
    steps = jnp.arange(side)
    hi = (tok // side)[..., None] == steps
    lo = (tok % side)[..., None] == steps
    hist = jnp.einsum('tph,tpl->thl', hi.astype(BF16), lo.astype(BF16), preferred_element_type=F32)
    seen = (hist > 0).astype(BF16)
    upto = (steps[:, None] <= steps[None, :]).astype(BF16)
    within = jnp.einsum('thl,lk->thk', seen, upto, preferred_element_type=F32)
    before = jnp.sum(jnp.where(steps[None, :, None] > steps[None, None, :], within[:, None, :, -1], 0.0), axis=-1)
    count = within + before[..., None]
    row = jnp.einsum('tph,thl->tpl', hi.astype(BF16), within.astype(BF16), preferred_element_type=F32)
    start = jnp.sum(jnp.where(hi, before[:, None, :], 0.0), axis=-1)
    place = (jnp.sum(jnp.where(lo, row, 0.0), axis=-1) + start - 1.0).astype(jnp.int32)
    places = jnp.arange(distinct, dtype=F32)
    hi_list = jnp.sum((count[:, None, :, -1] <= places[None, :, None]).astype(jnp.int32), axis=-1)
    in_row = hi_list[..., None] == steps
    row = jnp.einsum('tsh,thl->tsl', in_row.astype(BF16), within.astype(BF16), preferred_element_type=F32)
    start = jnp.sum(jnp.where(in_row, before[:, None, :], 0.0), axis=-1)
    lo_list = jnp.sum((row + start[..., None] <= places[None, :, None]).astype(jnp.int32), axis=-1)
    return hi_list * side + lo_list, place


def after(value, *earlier):
    return lax.optimization_barrier((value, *earlier))[0]


def solution(mesh):
    group = mesh.shape['ep']

    def permute(value, mask):
        return lax.ppermute(value, 'ep', [(i, i ^ mask) for i in range(group)])

    def dispatch(rows, masks):
        return [permute(rows[m], m) if m else rows[m] for m in masks]

    def device_step(x, gate_w, up_w, down_w, expert_picks, loss_w):
        tokens, cols = x.shape
        experts = gate_w.shape[1]
        local, capacity = expert_picks.shape
        picks = capacity // group
        distinct = local * picks // 2
        scale = 1.0 / math.sqrt(tokens * group * cols)
        me = lax.axis_index('ep')
        order = me ^ jnp.arange(group)
        gate_pad = jnp.pad(gate_w, ((0, 0), (0, LANES - experts)))

        wanted = expert_picks.reshape(local, group, picks)
        asked = lax.all_to_all(wanted, 'ep', 1, 1, tiled=True) - me * tokens
        asked = jnp.take(asked, order, axis=1).transpose(1, 0, 2)
        wanted = (jnp.take(wanted, order, axis=1) - (order * tokens)[None, :, None]).transpose(1, 0, 2)

        half = local // 2
        part_a = (up_w[:half], down_w[:half])
        xa, ya = [permute(v, 2) for v in part_a], [permute(v, 4) for v in part_a]
        partner = [permute(up_w, 1), permute(down_w, 1)]

        send_list, _ = rank_picks(asked.reshape(group, -1), distinct)
        spans = [(0, 0, local), (1, 0, local)] + [(m, 0, half) for m in (2, 4, 3, 5)]
        early = sum(s[2] for s in spans)
        spans += [(m, half, half) for m in (2, 4, 3, 5)] + [(6, 0, half), (7, 0, half), (6, half, half), (7, half, half)]
        ids_by_mask = order[:, None] * local + jnp.arange(local)[None, :]
        own_ids = jnp.concatenate([ids_by_mask[m, s:s + n] for m, s, n in spans])
        own_tok = jnp.concatenate([asked[m, s:s + n] for m, s, n in spans]).reshape(-1)
        own_idx = row_base(own_tok)
        gather_idx = jnp.concatenate([row_base(send_list).reshape(-1), own_idx])
        *send_x, picked_x = gather_rows(gather_idx, [x], gather_idx.size, group)
        *send_r, picked_r = gather_rows(after(gather_idx, picked_x), [loss_w], gather_idx.size, group)
        near, far = range(6), range(6, group)
        got_x, near_r, far_r = dispatch(send_x, range(group)), dispatch(send_r, near), dispatch(send_r, far)

        part_b = [w[half:] for w in after((up_w, down_w), picked_r)]
        xb, yb = [permute(v, 2) for v in part_b], [permute(v, 4) for v in part_b]

        def relay(vx, vy):
            return [permute(vx[0], 4), permute(vy[1], 2)]

        da, db = relay(xa, ya), relay(xb, yb)
        xa1, ya1, xb1, yb1, da1, db1 = ([permute(v, 1) for v in vs] for vs in (xa, ya, xb, yb, da, db))

        def owner(bufs, first, *pairs):
            ids = after(own_ids, bufs[2]) if bufs else own_ids
            return owner_group(ids, picked_x, picked_r, pairs, gate_pad, bufs, first, picks, experts, scale)

        bufs = owner([], 0, (up_w, down_w))
        bufs = owner(bufs, local, partner)
        bufs = owner(bufs, 2 * local, xa, ya, xa1, ya1)

        _, place = rank_picks(wanted.reshape(group, -1), distinct)
        rows_idx = row_base(place.reshape(group, local, picks) + jnp.arange(group)[:, None, None] * distinct)
        near_idx, far_idx = (rows_idx[r.start:r.stop].transpose(1, 0, 2).reshape(-1) for r in (near, far))
        my_ids = me * local + jnp.arange(local)
        *accs, probs = combine_first(after(own_idx, bufs[2]), own_tok, x, loss_w, *bufs, gate_pad, picks, early, experts, scale)
        both_idx = jnp.concatenate([near_idx, far_idx])
        rows_x = gather_rows(after(both_idx, accs[2]), got_x, local * capacity)
        near_rows = gather_rows(after(near_idx, rows_x), near_r, near_idx.size)
        sums = expert_grads(my_ids, rows_x, 0, near_rows, up_w, down_w, gate_pad, [], F32, experts, scale)

        own_ids = after(own_ids, sums[1])
        bufs = owner(bufs, 4 * local, xb, yb)
        bufs = owner(bufs, 5 * local, xb1, yb1)
        accs = combine_mid(own_idx, own_tok, *bufs, accs, picks, early, 2 * local)
        own_ids = after(own_ids, accs[2])
        bufs = owner(bufs, 6 * local, da)
        bufs = owner(bufs, 6 * local + half, da1)
        bufs = owner(bufs, 7 * local, db)
        y, grad_x, part = combine_last(own_ids, own_idx, own_tok, x, loss_w, picked_x, picked_r, *db1, *bufs, gate_pad,
                                       accs, probs, picks, 6 * local, experts, scale)
        part = part + permute(part, 1)
        far_rows = gather_rows(after(far_idx - row_base(far.start * distinct), part), far_r, far_idx.size)
        grad_up, grad_down = expert_grads(my_ids, rows_x, near_idx.size, far_rows, up_w, down_w, gate_pad, sums, BF16,
                                          experts, scale)
        others = [permute(part, mask) for mask in (2, 4, 6)]
        part = (part + others[0]) + (others[1] + others[2])
        return y, jnp.sum(part[experts:]) * scale, grad_x, grad_up, grad_down, part[:experts].T

    return jax.shard_map(device_step, mesh=mesh,
                         in_specs=(P('ep'), P(), P('ep'), P('ep'), P('ep'), P('ep')),
                         out_specs=(P('ep'), P(), P('ep'), P('ep'), P('ep'), P()),
                         check_vma=False)
```
